32 devices in a mesh: mkt: 8 (over y, x, core), trade: 1, scen: 4 (over z).
Axes of the slice: x: 2, y: 2, z: 4, core: 2. Of those that a mesh axis runs over, the one named last changes fastest.
Arguments:
- quotes: bfloat16 [512, 512], P('mkt'), may hold values from -6 to 6
- kernel: bfloat16 [64, 128, 128], P(('trade', 'scen')), may hold values from -0.5 to 0.5
- trade_block: int32 [2048], P('trade'), may hold values from 0 to 63
- trade_embed: bfloat16 [2048, 256], P('trade'), may hold values from -6 to 6
- position: float32 [2048], P('trade'), may hold values from -0.125 to 0.125
- scen_rank: int32 [512], P(('mkt', 'scen')), may hold values from 0 to 511, each once
- w_in: bfloat16 [128, 256], replicated, may hold values from -0.5 to 0.5
- w_mid: bfloat16 [256, 256], replicated, may hold values from -0.375 to 0.375
- b_mid: float32 [256], replicated, may hold values from -6 to 6
- w_out: bfloat16 [256], replicated, may hold values from -0.375 to 0.375
Outputs:
- book_pnl: float32 [512], P(('mkt', 'scen'))
- marginal: float32 [2048], P('trade')
- shortfall: float32 [], replicated
The draws below stay inside these ranges and needn't reach their ends.
Inputs may be any that keep to these rules, and one draw needn't show every extreme that they name: scen_rank holds each rank of 0 to 511 once.
All inputs are finite; a program needn't handle non-finite values.
Results may differ from the reference program's by a relative error of at most 0.014.
The reference program's roundings to bfloat16 on the way count: a program that leaves them out, or rounds other values in their place, can miss the bound.
Values may be sent and summed in bfloat16 or wider, within the bound.
No kernel may reach another device: no remote copies, remote signals or barrier semaphores. Data moves between devices by JAX's collectives and lax.ppermute only.
A program may use at most 64 MiB of HBM per device.

```python
import jax
import jax.numpy as jnp
from jax import lax

SEG = 128
WIN = 128
QSTEP = 8
HID = 256
NB = 64
Q = 512
S = 512
TRADES = 2048
RSPAN = 25


def with_ends(values, stream_key, low, high):
    extent = values.shape
    place = [jax.random.randint(jax.random.fold_in(stream_key, axis), (), 0, extent[axis]) for axis in range(len(extent))]
    values = values.at[tuple(place)].set(low)
    longest = extent.index(max(extent))
    place[longest] = (place[longest] + 1) % extent[longest]
    return values.at[tuple(place)].set(high)


def shard_levels(key, extent, cuts, smallest, high):
    level, own = 1.0, jax.random.fold_in(key, 6)
    for dim, blocks in cuts:
        draws = jnp.exp(jax.random.uniform(jax.random.fold_in(own, dim), (blocks,), jnp.float32, smallest / len(cuts), high / len(cuts)))
        level = level * jnp.repeat(draws, extent[dim] // blocks).reshape([-1 if axis == dim else 1 for axis in range(len(extent))])
    return level


def bell_draw(key, dims, width, limit, shards=(), held_as=jnp.bfloat16):
    level = shard_levels(key, dims, shards, -0.22, 0.18) if shards else 1.0
    drawn = jax.random.normal(key, dims, jnp.float32) * width * level
    return jnp.minimum(jnp.maximum(drawn, -limit), limit).astype(held_as)


def setup_inputs(seed: int = 0) -> dict:
    streams_of = jax.random.split(jax.random.key(seed), 11)
    return {
        "quotes": bell_draw(streams_of[0], (S, Q), 1.0, 6.0, ((0, 8),)),
        "kernel": bell_draw(streams_of[1], (NB, WIN, SEG), WIN ** -0.5, 0.5, ((0, 4),)),
        "trade_block": with_ends(jax.random.randint(streams_of[2], (TRADES,), 0, NB), jax.random.fold_in(streams_of[2], 1), 0, NB - 1).astype(jnp.int32),
        "trade_embed": bell_draw(streams_of[3], (TRADES, HID), 1.0, 6.0),
        "position": bell_draw(streams_of[4], (TRADES,), TRADES ** -0.5, 0.125, (), jnp.float32),
        "scen_rank": jax.random.permutation(streams_of[5], S).astype(jnp.int32),
        "w_in": bell_draw(streams_of[6], (SEG, HID), SEG ** -0.5, 0.5),
        "w_mid": bell_draw(streams_of[7], (HID, HID), HID ** -0.5, 0.375),
        "b_mid": bell_draw(streams_of[8], (HID,), 1.0, 6.0, (), jnp.float32),
        "w_out": bell_draw(streams_of[9], (HID,), HID ** -0.5, 0.375),
    }


def reference(quotes, kernel, trade_block, trade_embed, position, scen_rank, w_in, w_mid, b_mid, w_out):
    def build(block_pair):
        block_index, block_kernel = block_pair
        window_start = jnp.clip(QSTEP * block_index - (WIN - QSTEP) // 2, 0, Q - WIN).astype(jnp.int32)
        window = lax.dynamic_slice_in_dim(quotes, window_start, WIN, 1)
        return jnp.dot(window, block_kernel, preferred_element_type=jnp.float32).astype(jnp.bfloat16)

    states = lax.map(build, (jnp.arange(NB, dtype=jnp.int32), kernel))

    def price(scen_index):
        curve_table = lax.dynamic_index_in_dim(states, scen_index, 1, keepdims=False)
        trade_rows = curve_table[trade_block]
        hidden_one = jax.nn.silu(jnp.dot(trade_rows, w_in, preferred_element_type=jnp.float32) + trade_embed.astype(jnp.float32)).astype(jnp.bfloat16)
        hidden_two = jax.nn.silu(jnp.dot(hidden_one, w_mid, preferred_element_type=jnp.float32) + b_mid).astype(jnp.bfloat16)
        return jnp.dot(hidden_two, w_out, preferred_element_type=jnp.float32)

    values = lax.map(price, jnp.arange(S, dtype=jnp.int32))
    book_pnl = jnp.dot(values, position, precision=lax.Precision.HIGHEST)
    weight_sum = jnp.sum(jnp.exp(-jnp.arange(S, dtype=jnp.float32) / RSPAN))
    weights = jnp.exp(-scen_rank.astype(jnp.float32) / RSPAN) / weight_sum
    marginal = -jnp.dot(weights, values, precision=lax.Precision.HIGHEST)
    shortfall = -jnp.dot(weights, book_pnl, precision=lax.Precision.HIGHEST)
    return book_pnl, marginal, shortfall
```

```python
import functools

import jax
import jax.numpy as jnp
from jax import lax
from jax.experimental import pallas as pl
from jax.experimental.pallas import tpu as pltpu
from jax.sharding import PartitionSpec as P

QSTEP = 8
LANES = 128
SLOTS = 4
GROUP = 64
STEP = 4
BF = jnp.bfloat16
F32 = jnp.float32
NT = (((1,), (1,)), ((), ()))
HIGH = lax.Precision.HIGHEST


def iota(shape, dim):
    return lax.broadcasted_iota(jnp.int32, shape, dim)


def split3(x):
    high = x.astype(BF)
    rest = x - high.astype(F32)
    mid = rest.astype(BF)
    low = (rest - mid.astype(F32)).astype(BF)
    return high.astype(F32), mid.astype(F32), low.astype(F32)


def build_states(first, quotes_ref, kernel_ref, emit):
    local_count, window, _ = kernel_ref.shape
    quote_count = quotes_ref.shape[1]
    lane = iota((1, window), 1)
    for j in range(local_count):
        start = jnp.clip(QSTEP * (first + j) - (window - QSTEP) // 2, 0, quote_count - window)
        tile = start // window
        back = window - (start - tile * window)
        after = jnp.minimum(tile + 1, quote_count // window - 1)
        low = quotes_ref[:, pl.ds(pl.multiple_of(tile * window, window), window)].astype(F32)
        high = quotes_ref[:, pl.ds(pl.multiple_of(after * window, window), window)].astype(F32)
        cut = jnp.where(lane < back, pltpu.roll(low, back, 1), pltpu.roll(high, back, 1)).astype(BF)
        emit(j, jnp.dot(cut, kernel_ref[j], preferred_element_type=F32).astype(BF))


def states_kernel(first_ref, quotes_ref, kernel_ref, out_ref):
    def emit(j, state):
        out_ref[j] = state

    build_states(first_ref[0], quotes_ref, kernel_ref, emit)


def price_kernel(fused, scen_size, local_count, span, total, *refs):
    block_ref, position_ref, b_mid_ref, w_out_ref, *refs = refs
    rank_refs, refs = refs[:scen_size], refs[scen_size:]
    embed_hbm, w_in_hbm, w_mid_hbm, *refs = refs
    sources, refs = (refs[:2], refs[2:]) if fused else (refs[:1], refs[1:])
    send_ref, embed_ref, w_in_ref, w_mid_ref, *refs = refs
    held, refs = (refs[:2], refs[2:]) if fused else (refs[:1], refs[1:])
    (pre_ref, embed32_ref, meta_ref, hot_ref, place_ref, index_ref, index_smem, listed_ref, value_ref, first_a, first_b,
     second_a, second_b, sum_ref, sems) = refs
    rows = block_ref.shape[0]
    trades = rows * LANES
    block_rows = SLOTS * GROUP
    _, scenarios, hidden = pre_ref.shape
    tile_rows = SLOTS * scenarios
    loads = []
    for n, (source, target) in enumerate(
        zip((*sources, w_in_hbm, embed_hbm, w_mid_hbm), (*held, w_in_ref, embed_ref, w_mid_ref))
    ):
        loads.append(pltpu.make_async_copy(source, target, sems.at[n]))
        loads[-1].start()
    z = lax.axis_index("scen")

    block = block_ref[...]
    group = block // local_count
    mine = group % scen_size == z
    slot = ((group // scen_size) * local_count + block % local_count).astype(F32)
    flag = jnp.where(mine, 1.0, 0.0)
    flag16 = flag.astype(BF)
    upper = jnp.where(iota((LANES, LANES), 0) < iota((LANES, LANES), 1), 1.0, 0.0).astype(BF)
    lower = jnp.where(iota((rows, rows), 0) > iota((rows, rows), 1), 1.0, 0.0).astype(BF)
    inside = jnp.dot(flag16, upper, preferred_element_type=F32)
    above = jnp.sum(jnp.dot(lower, flag16, preferred_element_type=F32), axis=1, keepdims=True)
    place_ref[...] = jnp.where(mine, inside + above, -1.0)
    count = jnp.sum(flag).astype(jnp.int32)
    blocks = pl.cdiv(count, block_rows)

    high, mid, low = split3(position_ref[...])
    line = iota((16, LANES), 0)
    column = iota((16, LANES), 1).astype(F32)
    for r in range(rows):
        one = slice(r, r + 1)
        packed = jnp.where(line == 0, slot[one], jnp.where(line == 1, float(r), column))
        packed = jnp.where(line == 3, high[one], packed)
        packed = jnp.where(line == 4, mid[one], packed)
        packed = jnp.where(line == 5, low[one], packed)
        meta_ref[:, r * LANES : (r + 1) * LANES] = packed.astype(BF)
    index_ref[...] = jnp.zeros_like(index_ref)

    def list_block(b, carry):
        row = iota((block_rows, LANES), 0)
        want = (b * block_rows + SLOTS * (row % GROUP) + row // GROUP).astype(F32)
        for r in range(rows):
            hit = place_ref[r : r + 1, :] == want
            hot_ref[b, :, r * LANES : (r + 1) * LANES] = jnp.where(hit, 1.0, 0.0).astype(BF)
        found = lax.dot_general(meta_ref[...], hot_ref[b], NT, preferred_element_type=F32)
        index = (found[0:1] * rows + found[1:2]) * LANES + found[2:3]
        index_ref[pl.ds(b, 1), :] = index.astype(jnp.int32)
        listed_ref[pl.ds(b, 1), :] = found[3:4] + found[4:5] + found[5:6]
        return carry

    lax.fori_loop(0, blocks, list_block, 0)
    copy = pltpu.make_async_copy(index_ref, index_smem, sems.at[len(loads)])
    copy.start()

    for load in loads[:-2]:
        load.wait()
    w_in = w_in_ref[...] * BF(0.5)

    def emit(j, state):
        pre_ref[j] = jnp.dot(state, w_in, preferred_element_type=F32)

    if fused:
        build_states(z * local_count, *held, emit)
    else:

        def each(j, carry):
            emit(j, held[0][j])
            return carry

        lax.fori_loop(0, held[0].shape[0], each, 0)
    loads[-2].wait()
    embed32_ref[...] = embed_ref[...].astype(F32) * 0.5
    value_ref[...] = jnp.zeros_like(value_ref)
    loads[-1].wait()
    w_mid_ref[...] = w_mid_ref[...] * BF(0.5)
    bias = b_mid_ref[...] * 0.5
    w_out = jnp.broadcast_to(w_out_ref[...], (16, hidden))
    copy.wait()

    def first_stage(step, out_ref):
        for t in range(STEP):
            tile = step * STEP + t
            for k in range(SLOTS):
                entry = index_smem[tile // GROUP, k * GROUP + tile % GROUP]
                half = pre_ref[entry // trades] + embed32_ref[pl.ds(entry % trades, 1), :]
                at = t * tile_rows + k * scenarios
                out_ref[at : at + scenarios, :] = (half * (jnp.tanh(half) + 1.0)).astype(BF)

    def second_stage(in_ref, out_ref):
        for t in range(STEP):
            at = slice(t * tile_rows, (t + 1) * tile_rows)
            half = jnp.dot(in_ref[at, :], w_mid_ref[...], preferred_element_type=F32) + bias
            out_ref[at, :] = (half * (jnp.tanh(half) + 1.0)).astype(BF)

    def third_stage(step, in_ref):
        for t in range(STEP):
            at = slice(t * tile_rows, (t + 1) * tile_rows)
            value = lax.dot_general(w_out, in_ref[at, :], NT, preferred_element_type=F32)
            value_ref[pl.ds(step * STEP + t, 1), :] = value[0:1]

    def price(pair, carry):
        third_stage(2 * pair, second_a)
        second_stage(first_b, second_b)
        first_stage(2 * pair, first_a)
        third_stage(2 * pair + 1, second_b)
        second_stage(first_a, second_a)
        first_stage(2 * pair + 1, first_b)
        return carry

    steps = pl.cdiv(count, SLOTS * STEP)
    lax.fori_loop(0, pl.cdiv(steps + 2, 2), price, 0)

    ranks = jnp.concatenate([ref[...] for ref in rank_refs] * SLOTS, axis=1).astype(F32)
    weight_sum = jnp.sum(jnp.exp(-iota((8, total), 1).astype(F32) / span), axis=1, keepdims=True)[0:1]
    weight = pltpu.roll(jnp.exp(-ranks / span) / weight_sum, z * rank_refs[0].shape[1], 1)
    own = iota((16, tile_rows), 0) == iota((16, tile_rows), 1) // scenarios
    weights = jnp.where(own, jnp.broadcast_to(weight, (16, tile_rows)), 0.0)
    sum_ref[...] = jnp.zeros_like(sum_ref)

    def weigh(b, book):
        value = value_ref[pl.ds(pl.multiple_of(b * GROUP + 2 * STEP, 8), GROUP), :]
        tail = lax.dot_general(weights, value, NT, precision=HIGH, preferred_element_type=F32)
        tail = jnp.concatenate([tail[k : k + 1, :] for k in range(SLOTS)], axis=1)
        stack = jnp.concatenate([*split3(tail), jnp.zeros((13, block_rows), F32)], axis=0).astype(BF)
        sum_ref[...] += jnp.dot(stack, hot_ref[b], preferred_element_type=F32)
        listed = listed_ref[pl.ds(b, 1), :]
        listed = jnp.concatenate(
            [listed[:, k * GROUP : (k + 1) * GROUP] for k in range(SLOTS)] + [jnp.zeros((16 - SLOTS, GROUP), F32)], axis=0
        )
        return book + jnp.dot(listed, value, precision=HIGH, preferred_element_type=F32)

    book = lax.fori_loop(0, blocks, weigh, jnp.zeros((16, tile_rows), F32))
    book = jnp.sum(jnp.where(own, book, 0.0), axis=0, keepdims=True)
    loss = -jnp.sum(book * weight, axis=1, keepdims=True)
    book = sum(book[:, k * scenarios : (k + 1) * scenarios] for k in range(SLOTS))
    tail = -(sum_ref[0:1] + sum_ref[1:2] + sum_ref[2:3])
    rest = jnp.zeros((1, send_ref.shape[2] - trades - scenarios - 1), F32)
    row = jnp.concatenate([tail, book, loss, rest], axis=1)
    for p in range(send_ref.shape[0]):
        send_ref[p] = row


def local(quotes, kernel, trade_block, trade_embed, position, scen_rank, w_in, w_mid, b_mid, w_out):
    trade_size, scen_size, mkt_size = lax.axis_size("trade"), lax.axis_size("scen"), lax.axis_size("mkt")
    local_count, window, points = kernel.shape
    scenarios = quotes.shape[0]
    trades, hidden = trade_embed.shape
    rows = trades // LANES
    quarter = scen_rank.shape[0]
    peers = mkt_size * scen_size
    total = quarter * peers
    rank_row = scen_rank.reshape(1, quarter)
    ranks = [rank_row]
    for k in range(scen_size - 1, 0, -1):
        ranks.append(lax.ppermute(rank_row, "scen", [(i, (i + k) % scen_size) for i in range(scen_size)]))

    vmem = pl.BlockSpec(memory_space=pltpu.VMEM)
    hbm = pl.BlockSpec(memory_space=pl.ANY)
    fused = trade_size == 1
    if fused:
        sources = (quotes, kernel)
    else:
        first = (lax.axis_index(("trade", "scen")) * local_count).astype(jnp.int32).reshape(1)
        states = pl.pallas_call(
            states_kernel,
            out_shape=jax.ShapeDtypeStruct((local_count, scenarios, points), BF),
            in_specs=[pl.BlockSpec(memory_space=pltpu.SMEM), vmem, vmem],
            out_specs=vmem,
            name="states",
        )(first, quotes, kernel)
        sources = (lax.all_gather(states, "trade", axis=0, tiled=True),)
    list_rows = trades // (SLOTS * GROUP)
    step_rows = STEP * SLOTS * scenarios
    width = -(-(trades + scenarios + 1) // LANES) * LANES
    send = pl.pallas_call(
        functools.partial(price_kernel, fused, scen_size, local_count, total // 20, total),
        out_shape=jax.ShapeDtypeStruct((peers, 1, width), F32),
        in_specs=[vmem] * (4 + scen_size) + [hbm] * (3 + len(sources)),
        out_specs=vmem,
        scratch_shapes=[
            pltpu.VMEM(trade_embed.shape, BF),
            pltpu.VMEM(w_in.shape, BF),
            pltpu.VMEM(w_mid.shape, BF),
            *(pltpu.VMEM(source.shape, BF) for source in sources),
            pltpu.VMEM((local_count * trade_size, scenarios, hidden), F32),
            pltpu.VMEM((trades, hidden), F32),
            pltpu.VMEM((16, trades), BF),
            pltpu.VMEM((list_rows, SLOTS * GROUP, trades), BF),
            pltpu.VMEM((rows, LANES), F32),
            pltpu.VMEM((list_rows + 1, SLOTS * GROUP), jnp.int32),
            pltpu.SMEM((list_rows + 1, SLOTS * GROUP), jnp.int32),
            pltpu.VMEM((list_rows, SLOTS * GROUP), F32),
            pltpu.VMEM((trades // SLOTS + 4 * STEP, SLOTS * scenarios), F32),
            *(pltpu.VMEM((step_rows, hidden), BF) for _ in range(4)),
            pltpu.VMEM((16, trades), F32),
            pltpu.SemaphoreType.DMA((8,)),
        ],
        name="price",
    )(
        trade_block.reshape(rows, LANES),
        position.reshape(rows, LANES),
        b_mid.reshape(1, hidden),
        w_out.reshape(1, hidden),
        *ranks,
        trade_embed,
        w_in,
        w_mid,
        *sources,
    )
    got = lax.all_to_all(send, ("mkt", "scen"), split_axis=0, concat_axis=0, tiled=True).reshape(peers, width)
    sums = jnp.sum(got, axis=0)
    corner = (lax.axis_index("mkt") * scen_size, trades + lax.axis_index("scen") * quarter)
    book_pnl = lax.psum(jnp.sum(lax.dynamic_slice(got, corner, (scen_size, quarter)), axis=0), "trade")
    shortfall = lax.psum(sums[trades + scenarios], "trade")
    return (book_pnl, sums[:trades], shortfall)


def solution(mesh):
    placed = (
        P("mkt", None),
        P(("trade", "scen"), None, None),
        P("trade"),
        P("trade", None),
        P("trade"),
        P(("mkt", "scen")),
        P(),
        P(),
        P(),
        P(),
    )
    return jax.shard_map(
        local,
        mesh=mesh,
        in_specs=placed,
        out_specs=(P(("mkt", "scen")), P("trade"), P()),
        check_vma=False,
    )
```

```python
import functools

import jax
import jax.numpy as jnp
from jax import lax
from jax.experimental import pallas as pl
from jax.experimental.pallas import tpu as pltpu
from jax.sharding import PartitionSpec as P

QSTEP = 8
LANES = 128
SLOTS = 4
GROUP = 256
STEP = 4
BF = jnp.bfloat16
F32 = jnp.float32
NT = (((1,), (1,)), ((), ()))
HIGH = lax.Precision.HIGHEST


def iota(shape, dim):
    return lax.broadcasted_iota(jnp.int32, shape, dim)


def split3(x):
    high = x.astype(BF)
    rest = x - high.astype(F32)
    mid = rest.astype(BF)
    low = (rest - mid.astype(F32)).astype(BF)
    return high.astype(F32), mid.astype(F32), low.astype(F32)


def build_states(first, quotes_ref, kernel_ref, emit):
    local_count, window, _ = kernel_ref.shape
    quote_count = quotes_ref.shape[1]
    lane = iota((1, window), 1)
    for j in range(local_count):
        start = jnp.clip(QSTEP * (first + j) - (window - QSTEP) // 2, 0, quote_count - window)
        tile = start // window
        back = window - (start - tile * window)
        after = jnp.minimum(tile + 1, quote_count // window - 1)
        low = quotes_ref[:, pl.ds(pl.multiple_of(tile * window, window), window)].astype(F32)
        high = quotes_ref[:, pl.ds(pl.multiple_of(after * window, window), window)].astype(F32)
        cut = jnp.where(lane < back, pltpu.roll(low, back, 1), pltpu.roll(high, back, 1)).astype(BF)
        emit(j, jnp.dot(cut, kernel_ref[j], preferred_element_type=F32).astype(BF))


def states_kernel(first_ref, quotes_ref, kernel_ref, out_ref):
    def emit(j, state):
        out_ref[j] = state

    build_states(first_ref[0], quotes_ref, kernel_ref, emit)


def lanes_of(table, index):
    return jnp.take_along_axis(table, index, axis=1)


def price_kernel(fused, scen_size, local_count, span, total, *refs):
    rank_refs, refs = refs[:scen_size], refs[scen_size:]
    loaded = 9 if fused else 8
    origin, (send_ref, *refs) = refs[:loaded], refs[loaded:]
    copies, refs = refs[:loaded], refs[loaded:]
    block_ref, position_ref, *sources, w_in_ref, embed_ref, b_mid_ref, w_mid_ref, w_out_ref = copies
    pre_ref, embed32_ref, index_ref, index_smem, weighted_ref, value_ref, first_a, first_b, second_a, second_b, sems = refs
    loads = [pltpu.make_async_copy(here, there, sems.at[n]) for n, (here, there) in enumerate(zip(origin, copies))]
    for load in loads:
        load.start()
    rows = block_ref.shape[0]
    trades = rows * LANES
    _, scenarios, hidden = pre_ref.shape
    tile_rows = SLOTS * scenarios
    z = lax.axis_index("scen")
    loads[0].wait()
    loads[1].wait()

    block = block_ref[...]
    group = block // local_count
    mine = group % scen_size == z
    slot = (group // scen_size) * local_count + block % local_count
    flag = jnp.where(mine, 1.0, 0.0).astype(BF)
    upper = jnp.where(iota((LANES, LANES), 0) <= iota((LANES, LANES), 1), 1.0, 0.0).astype(BF)
    lower = jnp.where(iota((rows, rows), 0) > iota((rows, rows), 1), 1.0, 0.0).astype(BF)
    upto = jnp.dot(flag, upper, preferred_element_type=F32)
    above = jnp.sum(jnp.dot(lower, flag, preferred_element_type=F32), axis=1, keepdims=True)
    through = (above + upto[:, LANES - 1 :]).astype(jnp.int32)
    place = (upto + above).astype(jnp.int32) - 1
    above = above.astype(jnp.int32)
    count = jnp.sum(flag.astype(F32)).astype(jnp.int32)
    lane = iota((rows, LANES), 1)
    line = iota((rows, LANES), 0)
    want = (lane + 1).astype(F32)
    found = jnp.zeros((rows, LANES), jnp.int32)
    bit = LANES // 2
    while bit:
        found = jnp.where(lanes_of(upto, found + (bit - 1)) < want, found + bit, found)
        bit //= 2
    entry = lanes_of(slot, found) * trades + line * LANES + found
    placed = lanes_of(position_ref[...], found)
    cuts = rows // SLOTS
    spot = ((line % cuts) * LANES + lane) * SLOTS + line // cuts
    listed, weighted = jnp.zeros((rows, LANES), jnp.int32), jnp.zeros((rows, LANES), F32)
    for r in range(rows):
        one = slice(r, r + 1)
        here = (spot >= above[one]) & (spot < through[one])
        at = (spot - above[one]) & (LANES - 1)
        listed = jnp.where(here, lanes_of(jnp.broadcast_to(entry[one], (rows, LANES)), at), listed)
        weighted = jnp.where(here, lanes_of(jnp.broadcast_to(placed[one], (rows, LANES)), at), weighted)
    index_ref[:rows, :] = listed
    weighted_ref[...] = weighted
    index_ref[rows:, :] = jnp.zeros((8, LANES), jnp.int32)
    copy = pltpu.make_async_copy(index_ref, index_smem, sems.at[loaded])
    copy.start()
    for load in loads[2:-4]:
        load.wait()

    w_in = w_in_ref[...] * BF(0.5)

    def emit(j, state):
        pre_ref[j] = jnp.dot(state, w_in, preferred_element_type=F32)

    if fused:
        build_states(z * local_count, *sources, emit)
    else:

        def each(j, carry):
            emit(j, sources[0][j])
            return carry

        lax.fori_loop(0, sources[0].shape[0], each, 0)
    for load in loads[-4:]:
        load.wait()
    embed32_ref[...] = embed_ref[...].astype(F32) * 0.5
    value_ref[...] = jnp.zeros_like(value_ref)
    w_mid_ref[...] = w_mid_ref[...] * BF(0.5)
    bias = b_mid_ref[...] * 0.5
    w_out = jnp.broadcast_to(w_out_ref[...].reshape(1, hidden), (16, hidden))
    copy.wait()

    def first_stage(step, out_ref):
        for t in range(STEP):
            tile = step * STEP + t
            for k in range(SLOTS):
                chosen = index_smem[k * cuts + tile // LANES, tile % LANES]
                half = pre_ref[chosen // trades] + embed32_ref[pl.ds(chosen % trades, 1), :]
                at = (t * SLOTS + k) * scenarios
                out_ref[at : at + scenarios, :] = (half * (jnp.tanh(half) + 1.0)).astype(BF)

    def second_stage(in_ref, out_ref):
        for t in range(STEP):
            at = slice(t * tile_rows, (t + 1) * tile_rows)
            half = jnp.dot(in_ref[at, :], w_mid_ref[...], preferred_element_type=F32) + bias
            out_ref[at, :] = (half * (jnp.tanh(half) + 1.0)).astype(BF)

    def third_stage(step, in_ref):
        for t in range(STEP):
            at = slice(t * tile_rows, (t + 1) * tile_rows)
            value = lax.dot_general(w_out, in_ref[at, :], NT, preferred_element_type=F32)
            value_ref[pl.ds(step * STEP + t, 1), :] = value[0:1]

    def price(pair, carry):
        first_stage(2 * pair, first_a)
        second_stage(first_b, second_b)
        third_stage(2 * pair, second_a)
        first_stage(2 * pair + 1, first_b)
        second_stage(first_a, second_a)
        third_stage(2 * pair + 1, second_b)
        return carry

    steps = pl.cdiv(count, SLOTS * STEP)
    lax.fori_loop(0, pl.cdiv(steps + 2, 2), price, 0)

    ranks = jnp.concatenate([ref[...] for ref in rank_refs] * SLOTS, axis=1).astype(F32)
    weight_sum = jnp.sum(jnp.exp(-iota((8, total), 1).astype(F32) / span), axis=1, keepdims=True)[0:1]
    weight = pltpu.roll(jnp.exp(-ranks / span) / weight_sum, z * rank_refs[0].shape[1], 1)
    own = iota((8, tile_rows), 0) == iota((8, tile_rows), 1) // scenarios
    weights = jnp.where(own, jnp.broadcast_to(weight, (8, tile_rows)), 0.0)

    def weigh(b, carry):
        tail, book = carry
        value = value_ref[pl.ds(pl.multiple_of(b * GROUP + 2 * STEP, 8), GROUP), :]
        sums = lax.dot_general(weights, value, NT, precision=HIGH, preferred_element_type=F32)
        tile = place // SLOTS - b * GROUP
        for k in range(SLOTS):
            for j in range(GROUP // LANES):
                row = jnp.broadcast_to(sums[k : k + 1, j * LANES : (j + 1) * LANES], (rows, LANES))
                here = (place % SLOTS == k) & (tile // LANES == j) & mine
                tail = jnp.where(here, lanes_of(row, tile % LANES), tail)
        take = [
            jnp.concatenate([weighted_ref[pl.ds(k * cuts + b * (GROUP // LANES) + j, 1), :] for j in range(GROUP // LANES)], axis=1)
            for k in range(SLOTS)
        ]
        placed = jnp.concatenate([*take, jnp.zeros((8 - SLOTS, GROUP), F32)], axis=0)
        return tail, book + jnp.dot(placed, value, precision=HIGH, preferred_element_type=F32)

    tail, book = lax.fori_loop(
        0, pl.cdiv(count, SLOTS * GROUP), weigh, (jnp.zeros((rows, LANES), F32), jnp.zeros((8, tile_rows), F32))
    )
    book = jnp.sum(jnp.where(own, book, 0.0), axis=0, keepdims=True)
    loss = -jnp.sum(book * weight, axis=1, keepdims=True)
    book = sum(book[:, k * scenarios : (k + 1) * scenarios] for k in range(SLOTS))
    book = jnp.concatenate([book, loss, jnp.zeros((1, LANES - scenarios - 1), F32)], axis=1)
    out = jnp.concatenate([-tail, *split3(book), jnp.zeros((5, LANES), F32)], axis=0).astype(BF)
    for p in range(send_ref.shape[0]):
        send_ref[p] = out


def total_kernel(scen_size, quarter, got_ref, book_ref, marginal_ref, loss_ref):
    rows = marginal_ref.shape[0]
    scenarios = scen_size * quarter
    sums = jnp.sum(got_ref[...].astype(F32), axis=0)
    marginal_ref[...] = sums[:rows]
    book = got_ref[pl.ds(lax.axis_index("mkt") * scen_size, scen_size)].astype(F32)
    book = jnp.sum(jnp.sum(book, axis=0)[rows:], axis=0, keepdims=True)
    back = LANES - lax.axis_index("scen") * quarter
    book_ref[...] = pltpu.roll(book, back, 1)[:, :quarter]
    loss_ref[...] = jnp.sum(sums[rows:, scenarios : scenarios + 1], axis=0, keepdims=True)


def local(quotes, kernel, trade_block, trade_embed, position, scen_rank, w_in, w_mid, b_mid, w_out):
    trade_size, scen_size, mkt_size = lax.axis_size("trade"), lax.axis_size("scen"), lax.axis_size("mkt")
    local_count, window, points = kernel.shape
    scenarios = quotes.shape[0]
    trades, hidden = trade_embed.shape
    rows = trades // LANES
    quarter = scen_rank.shape[0]
    peers = mkt_size * scen_size
    total = quarter * peers
    rank_row = scen_rank.reshape(1, quarter)
    ranks = [rank_row]
    for k in range(scen_size - 1, 0, -1):
        ranks.append(lax.ppermute(rank_row, "scen", [(i, (i + k) % scen_size) for i in range(scen_size)]))

    vmem = pl.BlockSpec(memory_space=pltpu.VMEM)
    smem = pl.BlockSpec(memory_space=pltpu.SMEM)

    hbm = pl.BlockSpec(memory_space=pl.ANY)

    def held(x):
        return pltpu.with_memory_space_constraint(x, pltpu.VMEM)

    fused = trade_size == 1
    if fused:
        sources = (quotes, kernel)
    else:
        first = (lax.axis_index(("trade", "scen")) * local_count).astype(jnp.int32).reshape(1)
        states = pl.pallas_call(
            states_kernel,
            out_shape=jax.ShapeDtypeStruct((local_count, scenarios, points), BF),
            in_specs=[smem, vmem, vmem],
            out_specs=vmem,
            name="states",
        )(first, quotes, kernel)
        sources = (lax.all_gather(states, "trade", axis=0, tiled=True),)
    step_rows = STEP * SLOTS * scenarios
    tiles = -(-(trades // SLOTS + 4 * STEP) // LANES) * LANES
    inputs = (
        trade_block.reshape(rows, LANES), position.reshape(rows, LANES), *sources, w_in, trade_embed,
        b_mid.reshape(1, hidden), w_mid, w_out,
    )
    send = pl.pallas_call(
        functools.partial(price_kernel, fused, scen_size, local_count, total // 20, total),
        out_shape=pltpu.VMEM((peers, rows + 8, LANES), BF),
        in_specs=[vmem] * scen_size + [hbm] * len(inputs),
        out_specs=vmem,
        scratch_shapes=[
            *(pltpu.VMEM(x.shape, x.dtype) for x in inputs),
            pltpu.VMEM((local_count * trade_size, scenarios, hidden), F32),
            pltpu.VMEM((trades, hidden), F32),
            pltpu.VMEM((rows + 8, LANES), jnp.int32),
            pltpu.SMEM((rows + 8, LANES), jnp.int32),
            pltpu.VMEM((rows, LANES), F32),
            pltpu.VMEM((tiles, SLOTS * scenarios), F32),
            *(pltpu.VMEM((step_rows, hidden), BF) for _ in range(4)),
            pltpu.SemaphoreType.DMA((len(inputs) + 1,)),
        ],
        name="price",
    )(*(held(rank) for rank in ranks), *inputs)
    got = lax.all_to_all(send, ("mkt", "scen"), split_axis=0, concat_axis=0, tiled=True)
    book_pnl, marginal, shortfall = pl.pallas_call(
        functools.partial(total_kernel, scen_size, quarter),
        out_shape=(
            jax.ShapeDtypeStruct((1, quarter), F32),
            jax.ShapeDtypeStruct((rows, LANES), F32),
            jax.ShapeDtypeStruct((1, 1), F32),
        ),
        in_specs=[vmem],
        out_specs=(vmem, vmem, vmem),
        name="total",
    )(held(got))
    book_pnl = lax.psum(book_pnl.reshape(quarter), "trade")
    shortfall = lax.psum(shortfall.reshape(()), "trade")
    return (book_pnl, marginal.reshape(trades), shortfall)


def solution(mesh):
    placed = (
        P("mkt", None),
        P(("trade", "scen"), None, None),
        P("trade"),
        P("trade", None),
        P("trade"),
        P(("mkt", "scen")),
        P(),
        P(),
        P(),
        P(),
    )
    return jax.shard_map(
        local,
        mesh=mesh,
        in_specs=placed,
        out_specs=(P(("mkt", "scen")), P("trade"), P()),
        check_vma=False,
    )
```

```python
import functools

import jax
import jax.numpy as jnp
from jax import lax
from jax.experimental import pallas as pl
from jax.experimental.pallas import tpu as pltpu
from jax.sharding import PartitionSpec as P

QSTEP = 8
LANES = 128
SLOTS = 4
GROUP = 256
STEP = 8
BF = jnp.bfloat16
F32 = jnp.float32
NT = (((1,), (1,)), ((), ()))
HIGH = lax.Precision.HIGHEST


def iota(shape, dim):
    return lax.broadcasted_iota(jnp.int32, shape, dim)


def split3(x):
    high = x.astype(BF)
    rest = x - high.astype(F32)
    mid = rest.astype(BF)
    low = (rest - mid.astype(F32)).astype(BF)
    return high.astype(F32), mid.astype(F32), low.astype(F32)


def build_states(first, quotes_ref, kernel_ref, emit):
    local_count, window, _ = kernel_ref.shape
    quote_count = quotes_ref.shape[1]
    lane = iota((1, window), 1)
    for j in range(local_count):
        start = jnp.clip(QSTEP * (first + j) - (window - QSTEP) // 2, 0, quote_count - window)
        tile = start // window
        back = window - (start - tile * window)
        after = jnp.minimum(tile + 1, quote_count // window - 1)
        low = quotes_ref[:, pl.ds(pl.multiple_of(tile * window, window), window)].astype(F32)
        high = quotes_ref[:, pl.ds(pl.multiple_of(after * window, window), window)].astype(F32)
        cut = jnp.where(lane < back, pltpu.roll(low, back, 1), pltpu.roll(high, back, 1)).astype(BF)
        emit(j, jnp.dot(cut, kernel_ref[j], preferred_element_type=F32).astype(BF))


def states_kernel(first_ref, quotes_ref, kernel_ref, out_ref):
    def emit(j, state):
        out_ref[j] = state

    build_states(first_ref[0], quotes_ref, kernel_ref, emit)


def lanes_of(table, index):
    return jnp.take_along_axis(table, index, axis=1)


def price_kernel(fused, scen_size, local_count, span, total, *refs):
    rank_refs, refs = refs[:scen_size], refs[scen_size:]
    loaded = 9 if fused else 8
    origin, (send_ref, *refs) = refs[:loaded], refs[loaded:]
    copies, refs = refs[:loaded], refs[loaded:]
    block_ref, position_ref, *sources, w_in_ref, embed_ref, b_mid_ref, w_mid_ref, w_out_ref = copies
    pre_ref, embed32_ref, index_ref, index_smem, weighted_ref, value_ref, first_a, first_b, second_a, second_b, sems = refs
    loads = [pltpu.make_async_copy(here, there, sems.at[n]) for n, (here, there) in enumerate(zip(origin, copies))]
    for load in loads:
        load.start()
    rows = block_ref.shape[0]
    trades = rows * LANES
    _, scenarios, hidden = pre_ref.shape
    tile_rows = SLOTS * scenarios
    z = lax.axis_index("scen")
    loads[0].wait()
    loads[1].wait()

    block = block_ref[...]
    group = block // local_count
    mine = group % scen_size == z
    slot = (group // scen_size) * local_count + block % local_count
    flag = jnp.where(mine, 1.0, 0.0).astype(BF)
    upper = jnp.where(iota((LANES, LANES), 0) <= iota((LANES, LANES), 1), 1.0, 0.0).astype(BF)
    lower = jnp.where(iota((rows, rows), 0) > iota((rows, rows), 1), 1.0, 0.0).astype(BF)
    upto = jnp.dot(flag, upper, preferred_element_type=F32)
    above = jnp.sum(jnp.dot(lower, flag, preferred_element_type=F32), axis=1, keepdims=True)
    through = (above + upto[:, LANES - 1 :]).astype(jnp.int32)
    place = (upto + above).astype(jnp.int32) - 1
    above = above.astype(jnp.int32)
    count = jnp.sum(flag.astype(F32)).astype(jnp.int32)
    lane = iota((rows, LANES), 1)
    line = iota((rows, LANES), 0)
    want = (lane + 1).astype(F32)
    found = jnp.zeros((rows, LANES), jnp.int32)
    bit = LANES // 2
    while bit:
        found = jnp.where(lanes_of(upto, found + (bit - 1)) < want, found + bit, found)
        bit //= 2
    entry = lanes_of(slot, found) * trades + line * LANES + found
    placed = lanes_of(position_ref[...], found)
    cuts = rows // SLOTS
    spot = ((line % cuts) * LANES + lane) * SLOTS + line // cuts
    listed, weighted = jnp.zeros((rows, LANES), jnp.int32), jnp.zeros((rows, LANES), F32)
    for r in range(rows):
        one = slice(r, r + 1)
        here = (spot >= above[one]) & (spot < through[one])
        at = (spot - above[one]) & (LANES - 1)
        listed = jnp.where(here, lanes_of(jnp.broadcast_to(entry[one], (rows, LANES)), at), listed)
        weighted = jnp.where(here, lanes_of(jnp.broadcast_to(placed[one], (rows, LANES)), at), weighted)
    index_ref[:rows, :] = listed
    weighted_ref[...] = weighted
    index_ref[rows:, :] = jnp.zeros((8, LANES), jnp.int32)
    copy = pltpu.make_async_copy(index_ref, index_smem, sems.at[loaded])
    copy.start()
    for load in loads[2:-4]:
        load.wait()

    w_in = w_in_ref[...] * BF(0.5)

    def emit(j, state):
        pre_ref[j] = jnp.dot(state, w_in, preferred_element_type=F32)

    if fused:
        build_states(z * local_count, *sources, emit)
    else:

        def each(j, carry):
            emit(j, sources[0][j])
            return carry

        lax.fori_loop(0, sources[0].shape[0], each, 0)
    for load in loads[-4:]:
        load.wait()
    embed32_ref[...] = embed_ref[...].astype(F32) * 0.5
    value_ref[...] = jnp.zeros_like(value_ref)
    w_mid_ref[...] = w_mid_ref[...] * BF(0.5)
    bias = b_mid_ref[...] * 0.5
    w_out = jnp.broadcast_to(w_out_ref[...].reshape(1, hidden), (16, hidden))
    copy.wait()

    def first_stage(step, out_ref):
        for t in range(STEP):
            tile = step * STEP + t
            for k in range(SLOTS):
                chosen = index_smem[k * cuts + tile // LANES, tile % LANES]
                half = pre_ref[chosen // trades] + embed32_ref[pl.ds(chosen % trades, 1), :]
                at = (t * SLOTS + k) * scenarios
                out_ref[at : at + scenarios, :] = (half * (jnp.tanh(half) + 1.0)).astype(BF)

    def second_stage(in_ref, out_ref):
        halves = jnp.dot(in_ref[...], w_mid_ref[...], preferred_element_type=F32)
        for t in range(STEP):
            at = slice(t * tile_rows, (t + 1) * tile_rows)
            half = halves[at] + bias
            out_ref[at, :] = (half * (jnp.tanh(half) + 1.0)).astype(BF)

    def third_stage(step, in_ref):
        for t in range(STEP):
            at = slice(t * tile_rows, (t + 1) * tile_rows)
            value = lax.dot_general(w_out, in_ref[at, :], NT, preferred_element_type=F32)
            value_ref[pl.ds((step + 1) * STEP + t, 1), :] = value[0:1]

    def price(pair, carry):
        first_stage(2 * pair + 1, first_b)
        second_stage(first_a, second_a)
        third_stage(2 * pair - 1, second_b)
        first_stage(2 * pair + 2, first_a)
        second_stage(first_b, second_b)
        third_stage(2 * pair, second_a)
        return carry

    pairs = pl.cdiv(count, SLOTS * STEP) // 2
    first_stage(0, first_a)
    lax.fori_loop(0, pairs, price, 0)
    second_stage(first_a, second_a)
    third_stage(2 * pairs - 1, second_b)
    third_stage(2 * pairs, second_a)

    ranks = jnp.concatenate([ref[...] for ref in rank_refs] * SLOTS, axis=1).astype(F32)
    weight_sum = jnp.sum(jnp.exp(-iota((8, total), 1).astype(F32) / span), axis=1, keepdims=True)[0:1]
    weight = pltpu.roll(jnp.exp(-ranks / span) / weight_sum, z * rank_refs[0].shape[1], 1)
    own = iota((8, tile_rows), 0) == iota((8, tile_rows), 1) // scenarios
    weights = jnp.where(own, jnp.broadcast_to(weight, (8, tile_rows)), 0.0)

    def weigh(b, carry):
        tail, book = carry
        value = value_ref[pl.ds(pl.multiple_of(b * GROUP + STEP, 8), GROUP), :]
        sums = lax.dot_general(weights, value, NT, precision=HIGH, preferred_element_type=F32)
        tile = place // SLOTS - b * GROUP
        for k in range(SLOTS):
            for j in range(GROUP // LANES):
                row = jnp.broadcast_to(sums[k : k + 1, j * LANES : (j + 1) * LANES], (rows, LANES))
                here = (place % SLOTS == k) & (tile // LANES == j) & mine
                tail = jnp.where(here, lanes_of(row, tile % LANES), tail)
        take = [
            jnp.concatenate([weighted_ref[pl.ds(k * cuts + b * (GROUP // LANES) + j, 1), :] for j in range(GROUP // LANES)], axis=1)
            for k in range(SLOTS)
        ]
        placed = jnp.concatenate([*take, jnp.zeros((8 - SLOTS, GROUP), F32)], axis=0)
        return tail, book + jnp.dot(placed, value, precision=HIGH, preferred_element_type=F32)

    tail, book = lax.fori_loop(
        0, pl.cdiv(count, SLOTS * GROUP), weigh, (jnp.zeros((rows, LANES), F32), jnp.zeros((8, tile_rows), F32))
    )
    book = jnp.sum(jnp.where(own, book, 0.0), axis=0, keepdims=True)
    loss = -jnp.sum(book * weight, axis=1, keepdims=True)
    book = sum(book[:, k * scenarios : (k + 1) * scenarios] for k in range(SLOTS))
    book = jnp.concatenate([book, loss, jnp.zeros((1, LANES - scenarios - 1), F32)], axis=1)
    out = jnp.concatenate([-tail, *split3(book), jnp.zeros((5, LANES), F32)], axis=0).astype(BF)
    for p in range(send_ref.shape[0]):
        send_ref[p] = out


def total_kernel(scen_size, quarter, got_ref, book_ref, marginal_ref, loss_ref):
    rows = marginal_ref.shape[0]
    scenarios = scen_size * quarter
    sums = jnp.sum(got_ref[...].astype(F32), axis=0)
    marginal_ref[...] = sums[:rows]
    book = got_ref[pl.ds(lax.axis_index("mkt") * scen_size, scen_size)].astype(F32)
    book = jnp.sum(jnp.sum(book, axis=0)[rows:], axis=0, keepdims=True)
    back = LANES - lax.axis_index("scen") * quarter
    book_ref[...] = pltpu.roll(book, back, 1)[:, :quarter]
    loss_ref[...] = jnp.sum(sums[rows:, scenarios : scenarios + 1], axis=0, keepdims=True)


def local(quotes, kernel, trade_block, trade_embed, position, scen_rank, w_in, w_mid, b_mid, w_out):
    trade_size, scen_size, mkt_size = lax.axis_size("trade"), lax.axis_size("scen"), lax.axis_size("mkt")
    local_count, window, points = kernel.shape
    scenarios = quotes.shape[0]
    trades, hidden = trade_embed.shape
    rows = trades // LANES
    quarter = scen_rank.shape[0]
    peers = mkt_size * scen_size
    total = quarter * peers
    rank_row = scen_rank.reshape(1, quarter)
    ranks = [rank_row]
    for k in range(scen_size - 1, 0, -1):
        ranks.append(lax.ppermute(rank_row, "scen", [(i, (i + k) % scen_size) for i in range(scen_size)]))

    vmem = pl.BlockSpec(memory_space=pltpu.VMEM)
    smem = pl.BlockSpec(memory_space=pltpu.SMEM)

    hbm = pl.BlockSpec(memory_space=pl.ANY)

    def held(x):
        return pltpu.with_memory_space_constraint(x, pltpu.VMEM)

    fused = trade_size == 1
    if fused:
        sources = (quotes, kernel)
    else:
        first = (lax.axis_index(("trade", "scen")) * local_count).astype(jnp.int32).reshape(1)
        states = pl.pallas_call(
            states_kernel,
            out_shape=jax.ShapeDtypeStruct((local_count, scenarios, points), BF),
            in_specs=[smem, vmem, vmem],
            out_specs=vmem,
            name="states",
        )(first, quotes, kernel)
        sources = (lax.all_gather(states, "trade", axis=0, tiled=True),)
    step_rows = STEP * SLOTS * scenarios
    tiles = -(-(trades // SLOTS + 4 * STEP) // LANES) * LANES
    inputs = (
        trade_block.reshape(rows, LANES), position.reshape(rows, LANES), *sources, w_in, trade_embed,
        b_mid.reshape(1, hidden), w_mid, w_out,
    )
    send = pl.pallas_call(
        functools.partial(price_kernel, fused, scen_size, local_count, total // 20, total),
        out_shape=pltpu.VMEM((peers, rows + 8, LANES), BF),
        in_specs=[vmem] * scen_size + [hbm] * len(inputs),
        out_specs=vmem,
        scratch_shapes=[
            *(pltpu.VMEM(x.shape, x.dtype) for x in inputs),
            pltpu.VMEM((local_count * trade_size, scenarios, hidden), F32),
            pltpu.VMEM((trades, hidden), F32),
            pltpu.VMEM((rows + 8, LANES), jnp.int32),
            pltpu.SMEM((rows + 8, LANES), jnp.int32),
            pltpu.VMEM((rows, LANES), F32),
            pltpu.VMEM((tiles, SLOTS * scenarios), F32),
            *(pltpu.VMEM((step_rows, hidden), BF) for _ in range(4)),
            pltpu.SemaphoreType.DMA((len(inputs) + 1,)),
        ],
        name="price",
    )(*(held(rank) for rank in ranks), *inputs)
    got = lax.all_to_all(send, ("mkt", "scen"), split_axis=0, concat_axis=0, tiled=True)
    book_pnl, marginal, shortfall = pl.pallas_call(
        functools.partial(total_kernel, scen_size, quarter),
        out_shape=(
            jax.ShapeDtypeStruct((1, quarter), F32),
            jax.ShapeDtypeStruct((rows, LANES), F32),
            jax.ShapeDtypeStruct((1, 1), F32),
        ),
        in_specs=[vmem],
        out_specs=(vmem, vmem, vmem),
        name="total",
    )(held(got))
    book_pnl = lax.psum(book_pnl.reshape(quarter), "trade")
    shortfall = lax.psum(shortfall.reshape(()), "trade")
    return (book_pnl, marginal.reshape(trades), shortfall)


def solution(mesh):
    placed = (
        P("mkt", None),
        P(("trade", "scen"), None, None),
        P("trade"),
        P("trade", None),
        P("trade"),
        P(("mkt", "scen")),
        P(),
        P(),
        P(),
        P(),
    )
    return jax.shard_map(
        local,
        mesh=mesh,
        in_specs=placed,
        out_specs=(P(("mkt", "scen")), P("trade"), P()),
        check_vma=False,
    )
```

```python
import functools

import jax
import jax.numpy as jnp
from jax import lax
from jax.experimental import pallas as pl
from jax.experimental.pallas import tpu as pltpu
from jax.sharding import PartitionSpec as P

QSTEP = 8
LANES = 128
SLOTS = 4
GROUP = 256
STEP = 8
BF = jnp.bfloat16
F32 = jnp.float32
NT = (((1,), (1,)), ((), ()))
HIGH = lax.Precision.HIGHEST


def iota(shape, dim):
    return lax.broadcasted_iota(jnp.int32, shape, dim)


def split3(x):
    high = x.astype(BF)
    rest = x - high.astype(F32)
    mid = rest.astype(BF)
    low = (rest - mid.astype(F32)).astype(BF)
    return high.astype(F32), mid.astype(F32), low.astype(F32)


def build_states(first, quotes_ref, kernel_ref, emit):
    local_count, window, _ = kernel_ref.shape
    quote_count = quotes_ref.shape[1]
    lane = iota((1, window), 1)
    for j in range(local_count):
        start = jnp.clip(QSTEP * (first + j) - (window - QSTEP) // 2, 0, quote_count - window)
        tile = start // window
        back = window - (start - tile * window)
        after = jnp.minimum(tile + 1, quote_count // window - 1)
        low = quotes_ref[:, pl.ds(pl.multiple_of(tile * window, window), window)].astype(F32)
        high = quotes_ref[:, pl.ds(pl.multiple_of(after * window, window), window)].astype(F32)
        cut = jnp.where(lane < back, pltpu.roll(low, back, 1), pltpu.roll(high, back, 1)).astype(BF)
        emit(j, jnp.dot(cut, kernel_ref[j], preferred_element_type=F32).astype(BF))


def states_kernel(first_ref, quotes_ref, kernel_ref, out_ref):
    def emit(j, state):
        out_ref[j] = state

    build_states(first_ref[0], quotes_ref, kernel_ref, emit)


def lanes_of(table, index):
    return jnp.take_along_axis(table, index, axis=1)


def price_kernel(fused, scen_size, local_count, *refs):
    loaded = 9 if fused else 8
    origin, (value_ref, weighted_ref, place_ref, *refs) = refs[:loaded], refs[loaded:]
    copies, refs = refs[:loaded], refs[loaded:]
    block_ref, position_ref, *sources, w_in_ref, embed_ref, b_mid_ref, w_mid_ref, w_out_ref = copies
    pre_ref, embed32_ref, index_ref, index_smem, first_a, first_b, second_a, second_b, sems = refs
    loads = [pltpu.make_async_copy(here, there, sems.at[n]) for n, (here, there) in enumerate(zip(origin, copies))]
    for load in loads:
        load.start()
    rows = block_ref.shape[0]
    trades = rows * LANES
    _, scenarios, hidden = pre_ref.shape
    tile_rows = SLOTS * scenarios
    z = lax.axis_index("scen")
    loads[0].wait()
    loads[1].wait()

    block = block_ref[...]
    group = block // local_count
    mine = group % scen_size == z
    slot = (group // scen_size) * local_count + block % local_count
    flag = jnp.where(mine, 1.0, 0.0).astype(BF)
    upper = jnp.where(iota((LANES, LANES), 0) <= iota((LANES, LANES), 1), 1.0, 0.0).astype(BF)
    lower = jnp.where(iota((rows, rows), 0) > iota((rows, rows), 1), 1.0, 0.0).astype(BF)
    upto = jnp.dot(flag, upper, preferred_element_type=F32)
    above = jnp.sum(jnp.dot(lower, flag, preferred_element_type=F32), axis=1, keepdims=True)
    through = (above + upto[:, LANES - 1 :]).astype(jnp.int32)
    place_ref[...] = jnp.where(mine, (upto + above).astype(jnp.int32) - 1, -1)
    above = above.astype(jnp.int32)
    count = jnp.sum(flag.astype(F32)).astype(jnp.int32)
    lane = iota((rows, LANES), 1)
    line = iota((rows, LANES), 0)
    want = (lane + 1).astype(F32)
    found = jnp.zeros((rows, LANES), jnp.int32)
    bit = LANES // 2
    while bit:
        found = jnp.where(lanes_of(upto, found + (bit - 1)) < want, found + bit, found)
        bit //= 2
    entry = lanes_of(slot, found) * trades + line * LANES + found
    placed = lanes_of(position_ref[...], found)
    cuts = rows // SLOTS
    spot = ((line % cuts) * LANES + lane) * SLOTS + line // cuts
    listed, weighted = jnp.zeros((rows, LANES), jnp.int32), jnp.zeros((rows, LANES), F32)
    for r in range(rows):
        one = slice(r, r + 1)
        here = (spot >= above[one]) & (spot < through[one])
        at = (spot - above[one]) & (LANES - 1)
        listed = jnp.where(here, lanes_of(jnp.broadcast_to(entry[one], (rows, LANES)), at), listed)
        weighted = jnp.where(here, lanes_of(jnp.broadcast_to(placed[one], (rows, LANES)), at), weighted)
    index_ref[:rows, :] = listed
    weighted_ref[...] = weighted
    index_ref[rows:, :] = jnp.zeros((8, LANES), jnp.int32)
    copy = pltpu.make_async_copy(index_ref, index_smem, sems.at[loaded])
    copy.start()
    for load in loads[2:-4]:
        load.wait()

    w_in = w_in_ref[...] * BF(0.5)

    def emit(j, state):
        pre_ref[j] = jnp.dot(state, w_in, preferred_element_type=F32)

    if fused:
        build_states(z * local_count, *sources, emit)
    else:

        def each(j, carry):
            emit(j, sources[0][j])
            return carry

        lax.fori_loop(0, sources[0].shape[0], each, 0)
    for load in loads[-4:]:
        load.wait()
    embed32_ref[...] = embed_ref[...].astype(F32) * 0.5
    value_ref[...] = jnp.zeros_like(value_ref)
    w_mid_ref[...] = w_mid_ref[...] * BF(0.5)
    bias = b_mid_ref[...] * 0.5
    w_out = jnp.broadcast_to(w_out_ref[...].reshape(1, hidden), (16, hidden))
    copy.wait()

    def first_stage(step, out_ref):
        for t in range(STEP):
            tile = step * STEP + t
            for k in range(SLOTS):
                chosen = index_smem[k * cuts + tile // LANES, tile % LANES]
                half = pre_ref[chosen // trades] + embed32_ref[pl.ds(chosen % trades, 1), :]
                at = (t * SLOTS + k) * scenarios
                out_ref[at : at + scenarios, :] = (half * (jnp.tanh(half) + 1.0)).astype(BF)

    def second_stage(in_ref, out_ref):
        halves = jnp.dot(in_ref[...], w_mid_ref[...], preferred_element_type=F32)
        for t in range(STEP):
            at = slice(t * tile_rows, (t + 1) * tile_rows)
            half = halves[at] + bias
            out_ref[at, :] = (half * (jnp.tanh(half) + 1.0)).astype(BF)

    def third_stage(step, in_ref):
        for t in range(STEP):
            at = slice(t * tile_rows, (t + 1) * tile_rows)
            value = lax.dot_general(w_out, in_ref[at, :], NT, preferred_element_type=F32)
            value_ref[pl.ds((step + 1) * STEP + t, 1), :] = value[0:1]

    def price(pair, carry):
        first_stage(2 * pair + 1, first_b)
        second_stage(first_a, second_a)
        third_stage(2 * pair - 1, second_b)
        first_stage(2 * pair + 2, first_a)
        second_stage(first_b, second_b)
        third_stage(2 * pair, second_a)
        return carry

    pairs = pl.cdiv(count, SLOTS * STEP) // 2
    first_stage(0, first_a)
    lax.fori_loop(0, pairs, price, 0)
    second_stage(first_a, second_a)
    third_stage(2 * pairs - 1, second_b)
    third_stage(2 * pairs, second_a)


def weigh_kernel(scen_size, span, total, *refs):
    value_ref, weighted_ref, place_ref, *rank_refs, send_ref = refs
    rows = place_ref.shape[0]
    tile_rows = value_ref.shape[1]
    scenarios = tile_rows // SLOTS
    cuts = rows // SLOTS
    z = lax.axis_index("scen")
    place = place_ref[...]
    mine = place >= 0
    count = jnp.sum(jnp.where(mine, 1.0, 0.0)).astype(jnp.int32)
    ranks = jnp.concatenate([ref[...] for ref in rank_refs] * SLOTS, axis=1).astype(F32)
    weight_sum = jnp.sum(jnp.exp(-iota((8, total), 1).astype(F32) / span), axis=1, keepdims=True)[0:1]
    weight = pltpu.roll(jnp.exp(-ranks / span) / weight_sum, z * rank_refs[0].shape[1], 1)
    own = iota((8, tile_rows), 0) == iota((8, tile_rows), 1) // scenarios
    weights = jnp.where(own, jnp.broadcast_to(weight, (8, tile_rows)), 0.0)

    def weigh(b, carry):
        tail, book = carry
        value = value_ref[pl.ds(pl.multiple_of(b * GROUP + STEP, 8), GROUP), :]
        sums = lax.dot_general(weights, value, NT, precision=HIGH, preferred_element_type=F32)
        tile = place // SLOTS - b * GROUP
        for k in range(SLOTS):
            for j in range(GROUP // LANES):
                row = jnp.broadcast_to(sums[k : k + 1, j * LANES : (j + 1) * LANES], (rows, LANES))
                here = (place % SLOTS == k) & (tile // LANES == j) & mine
                tail = jnp.where(here, lanes_of(row, tile % LANES), tail)
        take = [
            jnp.concatenate([weighted_ref[pl.ds(k * cuts + b * (GROUP // LANES) + j, 1), :] for j in range(GROUP // LANES)], axis=1)
            for k in range(SLOTS)
        ]
        placed = jnp.concatenate([*take, jnp.zeros((8 - SLOTS, GROUP), F32)], axis=0)
        return tail, book + jnp.dot(placed, value, precision=HIGH, preferred_element_type=F32)

    tail, book = lax.fori_loop(
        0, pl.cdiv(count, SLOTS * GROUP), weigh, (jnp.zeros((rows, LANES), F32), jnp.zeros((8, tile_rows), F32))
    )
    book = jnp.sum(jnp.where(own, book, 0.0), axis=0, keepdims=True)
    loss = -jnp.sum(book * weight, axis=1, keepdims=True)
    book = sum(book[:, k * scenarios : (k + 1) * scenarios] for k in range(SLOTS))
    book = jnp.concatenate([book, loss, jnp.zeros((1, LANES - scenarios - 1), F32)], axis=1)
    out = jnp.concatenate([-tail, *split3(book), jnp.zeros((5, LANES), F32)], axis=0).astype(BF)
    for p in range(send_ref.shape[0]):
        send_ref[p] = out


def total_kernel(scen_size, quarter, got_ref, book_ref, marginal_ref, loss_ref):
    rows = marginal_ref.shape[0]
    scenarios = scen_size * quarter
    sums = jnp.sum(got_ref[...].astype(F32), axis=0)
    marginal_ref[...] = sums[:rows]
    book = got_ref[pl.ds(lax.axis_index("mkt") * scen_size, scen_size)].astype(F32)
    book = jnp.sum(jnp.sum(book, axis=0)[rows:], axis=0, keepdims=True)
    back = LANES - lax.axis_index("scen") * quarter
    book_ref[...] = pltpu.roll(book, back, 1)[:, :quarter]
    loss_ref[...] = jnp.sum(sums[rows:, scenarios : scenarios + 1], axis=0, keepdims=True)


def local(quotes, kernel, trade_block, trade_embed, position, scen_rank, w_in, w_mid, b_mid, w_out):
    trade_size, scen_size, mkt_size = lax.axis_size("trade"), lax.axis_size("scen"), lax.axis_size("mkt")
    local_count, window, points = kernel.shape
    scenarios = quotes.shape[0]
    trades, hidden = trade_embed.shape
    rows = trades // LANES
    quarter = scen_rank.shape[0]
    peers = mkt_size * scen_size
    total = quarter * peers
    rank_row = scen_rank.reshape(1, quarter)
    ranks = [rank_row]
    for k in range(scen_size - 1, 0, -1):
        ranks.append(lax.ppermute(rank_row, "scen", [(i, (i + k) % scen_size) for i in range(scen_size)]))

    vmem = pl.BlockSpec(memory_space=pltpu.VMEM)
    smem = pl.BlockSpec(memory_space=pltpu.SMEM)

    hbm = pl.BlockSpec(memory_space=pl.ANY)

    def held(x):
        return pltpu.with_memory_space_constraint(x, pltpu.VMEM)

    fused = trade_size == 1
    if fused:
        sources = (quotes, kernel)
    else:
        first = (lax.axis_index(("trade", "scen")) * local_count).astype(jnp.int32).reshape(1)
        states = pl.pallas_call(
            states_kernel,
            out_shape=jax.ShapeDtypeStruct((local_count, scenarios, points), BF),
            in_specs=[smem, vmem, vmem],
            out_specs=vmem,
            name="states",
        )(first, quotes, kernel)
        sources = (lax.all_gather(states, "trade", axis=0, tiled=True),)
    step_rows = STEP * SLOTS * scenarios
    tiles = -(-(trades // SLOTS + 4 * STEP) // LANES) * LANES
    inputs = (
        trade_block.reshape(rows, LANES), position.reshape(rows, LANES), *sources, w_in, trade_embed,
        b_mid.reshape(1, hidden), w_mid, w_out,
    )
    value, weighted, place = pl.pallas_call(
        functools.partial(price_kernel, fused, scen_size, local_count),
        out_shape=(
            pltpu.VMEM((tiles, SLOTS * scenarios), F32),
            pltpu.VMEM((rows, LANES), F32),
            pltpu.VMEM((rows, LANES), jnp.int32),
        ),
        in_specs=[hbm] * len(inputs),
        out_specs=(vmem, vmem, vmem),
        scratch_shapes=[
            *(pltpu.VMEM(x.shape, x.dtype) for x in inputs),
            pltpu.VMEM((local_count * trade_size, scenarios, hidden), F32),
            pltpu.VMEM((trades, hidden), F32),
            pltpu.VMEM((rows + 8, LANES), jnp.int32),
            pltpu.SMEM((rows + 8, LANES), jnp.int32),
            *(pltpu.VMEM((step_rows, hidden), BF) for _ in range(4)),
            pltpu.SemaphoreType.DMA((len(inputs) + 1,)),
        ],
        cost_estimate=pl.CostEstimate(flops=10**10, transcendentals=0, bytes_accessed=2 * 10**6),
        name="price",
    )(*inputs)
    send = pl.pallas_call(
        functools.partial(weigh_kernel, scen_size, total // 20, total),
        out_shape=pltpu.VMEM((peers, rows + 8, LANES), BF),
        in_specs=[vmem] * (3 + scen_size),
        out_specs=vmem,
        name="weigh",
    )(held(value), held(weighted), held(place), *(held(rank) for rank in ranks))
    got = lax.all_to_all(send, ("mkt", "scen"), split_axis=0, concat_axis=0, tiled=True)
    book_pnl, marginal, shortfall = pl.pallas_call(
        functools.partial(total_kernel, scen_size, quarter),
        out_shape=(
            jax.ShapeDtypeStruct((1, quarter), F32),
            jax.ShapeDtypeStruct((rows, LANES), F32),
            jax.ShapeDtypeStruct((1, 1), F32),
        ),
        in_specs=[vmem],
        out_specs=(vmem, vmem, vmem),
        name="total",
    )(held(got))
    book_pnl = lax.psum(book_pnl.reshape(quarter), "trade")
    shortfall = lax.psum(shortfall.reshape(()), "trade")
    return (book_pnl, marginal.reshape(trades), shortfall)


def solution(mesh):
    placed = (
        P("mkt", None),
        P(("trade", "scen"), None, None),
        P("trade"),
        P("trade", None),
        P("trade"),
        P(("mkt", "scen")),
        P(),
        P(),
        P(),
        P(),
    )
    return jax.shard_map(
        local,
        mesh=mesh,
        in_specs=placed,
        out_specs=(P(("mkt", "scen")), P("trade"), P()),
        check_vma=False,
    )
```
